32 devices in a mesh: gy: 4 (over x, core), gx: 8 (over z, y).
Axes of the slice: x: 2, y: 2, z: 4, core: 2. Of those that a mesh axis runs over, the one named last changes fastest.
Arguments:
- first_factor: bfloat16 [4096, 2048], P('gy', 'gx'), may hold values from -6 to 6
- second_factor: bfloat16 [2048, 8192], P('gy', 'gx'), may hold values from -0.125 to 0.125
- result_in: float32 [4096, 8192], P('gy', 'gx'), may hold values from -6 to 6
- pivot_scale: float32 [2048], replicated, may hold values from 0.25 to 1.75
Outputs:
- corrected: float32 [4096, 8192], P('gy', 'gx')
The draws below stay inside these ranges and needn't reach their ends.
All inputs are finite; a program needn't handle non-finite values.
Results may differ from the reference program's by a relative error of at most 0.002.
Values may be sent and summed in bfloat16 or wider, within the bound.
A program may use at most 128 MiB of HBM per device.

```python
import jax
import jax.numpy as jnp
from jax import lax

ROWS = 4096
COLS = 8192
INNER = 2048


def levels(rng, dims, shards, low, largest):
    def one(dim, blocks):
        draws = jax.random.uniform(jax.random.fold_in(jax.random.fold_in(rng, 6), dim), (blocks,), jnp.float32, low / len(shards), largest / len(shards))
        return jnp.repeat(jnp.exp(draws), dims[dim] // blocks).reshape((-1,) + (1,) * (len(dims) - dim - 1))

    factor_of = one(*shards[0])
    for cut in shards[1:]:
        factor_of = factor_of * one(*cut)
    return factor_of


def centred(rng, extent, spread, most, pieces=(), held_as=jnp.bfloat16):
    loudness = levels(rng, extent, pieces, -0.22, 0.18) if pieces else 1.0
    drawn = jax.random.normal(rng, extent, jnp.float32) * spread * loudness
    return jnp.minimum(jnp.maximum(drawn, -most), most).astype(held_as)


def setup_inputs(seed: int = 0) -> dict:
    keys = jax.random.split(jax.random.key(seed), 5)
    first_factor = centred(keys[0], (ROWS, INNER), 1.0, 6.0, ((0, 4), (1, 8)))
    second_factor = centred(keys[1], (INNER, COLS), INNER ** -0.5, 0.125, ((0, 4), (1, 8)))
    result_in = centred(keys[2], (ROWS, COLS), 1.0, 6.0, ((0, 4), (1, 8)), jnp.float32)
    pivot_scale = jnp.clip(1.0 + 0.15 * jax.random.normal(keys[3], (INNER,), jnp.float32), 0.25, 1.75)
    return dict(first_factor=first_factor, second_factor=second_factor, result_in=result_in, pivot_scale=pivot_scale)


def reference(first_factor, second_factor, result_in, pivot_scale):
    scaled_left = (first_factor.astype(jnp.float32) * pivot_scale).astype(jnp.bfloat16)
    corrected = result_in - jnp.dot(scaled_left, second_factor, preferred_element_type=jnp.float32)
    row_power = lax.optimization_barrier(jnp.sum(corrected * corrected, axis=1))
    corrected = corrected * lax.rsqrt(row_power / COLS + 1e-06)[:, None]
    return corrected
```

```python
import functools

import jax
import jax.numpy as jnp
from jax import lax
from jax.experimental import pallas as pl
from jax.experimental.pallas import tpu as pltpu
from jax.sharding import PartitionSpec as P

MESH = pl.DeviceIdType.MESH
LANES = 128


def kernel(n_gx, n_gy, a_ref, b_ref, r_ref, p_ref, o_ref, abuf, bbuf, pbuf, pv,
           a_loc, b_loc, r_loc, p_loc, arecv, brecv, zs, zd, ys, xs, bcs, bxs, psend, precv):
    half, ka = abuf.shape[2], abuf.shape[3]
    nc = b_ref.shape[0] // ka
    line, xn = n_gx // 2, n_gy // 2
    gx, gy = lax.axis_index("gx"), lax.axis_index("gy")
    z, y = gx // 2, gx % 2
    x, core = gy // 2, gy % 2
    pair = z + 1 - 2 * (z % 2)
    total_cols = o_ref.shape[1] * n_gx

    def blk(zz, yy):
        return zz * 2 + yy

    up = {"gx": blk(jnp.minimum(z + 1, line - 1), y), "gy": gy}
    down = {"gx": blk(jnp.maximum(z - 1, 0), y), "gy": gy}
    side = {"gx": blk(z, 1 - y), "gy": gy}
    across = {"gx": blk(pair, y), "gy": gy}
    mate = {"gx": gx, "gy": x * 2 + 1 - core}

    def x_peer(dx):
        return ((x + dx) % xn) * 2 + core

    a_in = [pltpu.make_async_copy(a_ref.at[pl.ds(h * half, half)], abuf.at[gx, h], a_loc.at[h]) for h in range(2)]
    b_in = [pltpu.make_async_copy(b_ref.at[pl.ds(c * ka, ka)], bbuf.at[gy * nc + c], b_loc.at[c]) for c in range(nc)]
    p_in = pltpu.make_async_copy(p_ref, pv, p_loc)
    r_in = pltpu.make_async_copy(r_ref, o_ref, r_loc)
    for cp in a_in + b_in + [p_in, r_in]:
        cp.start()

    barrier = pltpu.get_barrier_semaphore()
    for d in range(1, n_gx):
        pl.semaphore_signal(barrier, inc=1, device_id={"gx": (gx + d) % n_gx, "gy": gy}, device_id_type=MESH)
    pl.semaphore_signal(barrier, inc=1, device_id=mate, device_id_type=MESH)
    for dx in range(1, xn):
        pl.semaphore_signal(barrier, inc=1, device_id={"gx": gx, "gy": x_peer(dx)}, device_id_type=MESH)
    pl.semaphore_wait(barrier, n_gx - 1 + 1 + xn - 1)

    def acopy(j, h, sem, dev):
        return pltpu.make_async_remote_copy(
            src_ref=abuf.at[j, h], dst_ref=abuf.at[j, h], send_sem=sem,
            recv_sem=arecv.at[j, h], device_id=dev, device_id_type=MESH)

    def bcopy(j, sem, dev):
        return pltpu.make_async_remote_copy(
            src_ref=bbuf.at[j], dst_ref=bbuf.at[j], send_sem=sem,
            recv_sem=brecv.at[j], device_id=dev, device_id_type=MESH)

    def a_arrived(j, h):
        acopy(j, h, xs, side).wait_recv()

    def b_arrived(j):
        bcopy(j, xs, mate).wait_recv()

    def to_side(zz, h):
        return acopy(blk(zz, y), h, ys.at[zz, h], side)

    def to_up(zz, h):
        return acopy(blk(zz, y), h, zs.at[zz, h], up)

    def to_down(zz, h):
        return acopy(blk(zz, y), h, zs.at[zz, h], down)

    def own_down(h):
        return acopy(gx, h, zd.at[h], down)

    def to_across():
        return acopy(blk(z, 1 - y), 1, xs, across)

    def to_mate(j):
        return bcopy(j, bcs.at[j], mate)

    def to_x(dx, c):
        return bcopy(gy * nc + c, bxs.at[(dx - 1) * nc + c], {"gx": gx, "gy": x_peer(dx)})

    has_up, has_down = z + 1 < line, z > 0

    for h in range(2):
        a_in[h].wait()
        to_side(z, h).start()
        pl.when(has_up)(lambda h=h: to_up(z, h).start())
        pl.when(has_down)(lambda h=h: own_down(h).start())
    for c in range(nc):
        b_in[c].wait()
        for dx in range(1, xn):
            to_x(dx, c).start()
        to_mate(gy * nc + c).start()

    def z_round(s, h):
        @pl.when(z - s >= 0)
        def _():
            zz = z - s
            a_arrived(blk(zz, y), h)
            pl.when(has_up)(lambda: to_up(zz, h).start())
            if h == 0 or s > 1:
                to_side(zz, h).start()
            else:
                pl.when(zz != pair)(lambda: to_side(zz, h).start())

        @pl.when(z + s < line)
        def _():
            zz = z + s
            a_arrived(blk(zz, y), h)
            pl.when(has_down)(lambda: to_down(zz, h).start())
            if h == 0 or s > 1:
                to_side(zz, h).start()
            else:
                pl.when(zz != pair)(lambda: to_side(zz, h).start())

    def side_wait(zz, h, s):
        if h == 0 or s != 1:
            a_arrived(blk(zz, 1 - y), h)
        else:
            pl.when(zz != pair)(lambda: a_arrived(blk(zz, 1 - y), h))

    def y_round(s):
        for h in range(2):
            if s == 0:
                side_wait(z, h, s)
            else:
                pl.when(z - s >= 0)(lambda h=h: side_wait(z - s, h, s))
                pl.when(z + s < line)(lambda h=h: side_wait(z + s, h, s))

    def b_round(c):
        for dx in range(1, xn):
            j = x_peer(dx) * nc + c
            b_arrived(j)
            to_mate(j).start()

    def unit(j, h):
        rows = pl.ds(pl.multiple_of(h * half, half), half)
        scale = pv[:, pl.ds(pl.multiple_of(j * ka, ka), ka)]
        left = (abuf[j, h].astype(jnp.float32) * scale).astype(jnp.bfloat16)
        o_ref[rows, :] = o_ref[rows, :] - jnp.dot(left, bbuf[j], preferred_element_type=jnp.float32)

    def compute(yy, pred):
        def body(t, carry):
            zz, h = t // 2, t % 2
            pl.when(pred(zz, h))(lambda: unit(blk(zz, yy), h))
            return carry
        lax.fori_loop(0, 2 * line, body, 0)

    def near(zz, s):
        return jnp.logical_and(zz - z <= s, z - zz <= s)

    for s in range(1, line - 1):
        if s >= 2:
            y_round(s - 2)
        for h in range(2):
            z_round(s, h)
        if s - 1 < nc:
            b_round(s - 1)
    for c in range(line - 2, nc):
        b_round(c)
    to_across().start()
    for c in range(nc):
        b_arrived(mate["gy"] * nc + c)
        for dx in range(1, xn):
            b_arrived((((x + dx) % xn) * 2 + 1 - core) * nc + c)
    p_in.wait()
    r_in.wait()

    compute(y, lambda zz, h: near(zz, line - 2))
    z_round(line - 1, 0)
    y_round(line - 3)
    compute(1 - y, lambda zz, h: jnp.logical_and(near(zz, line - 3), jnp.logical_or(zz != pair, h == 0)))
    z_round(line - 1, 1)
    compute(y, lambda zz, h: jnp.logical_not(near(zz, line - 2)))

    def late(s, h, when=None):
        exists = jnp.logical_or(z >= s, z + s < line)
        zz = jnp.where(z >= s, z - s, z + s)

        @pl.when(exists if when is None else jnp.logical_and(exists, when))
        def _():
            a_arrived(blk(zz, 1 - y), h)
            unit(blk(zz, 1 - y), h)

    tiles = half // LANES
    lane_tiles = o_ref.shape[1] // LANES

    def pcopy(h, peer):
        return pltpu.make_async_remote_copy(
            src_ref=pbuf.at[h, gx], dst_ref=pbuf.at[h, gx], send_sem=psend.at[h],
            recv_sem=precv.at[h], device_id={"gx": peer, "gy": gy}, device_id_type=MESH)

    def power(h):
        found = []
        for r in range(tiles):
            block = o_ref[pl.ds(h * half + r * LANES, LANES), :]
            part = jnp.zeros((LANES, LANES), jnp.float32)
            for t in range(lane_tiles):
                piece = block[:, t * LANES:(t + 1) * LANES]
                part = part + piece * piece
            found.append(jnp.sum(part.T, axis=0, keepdims=True))
        spare = pbuf.shape[2] - tiles
        if spare:
            found.append(jnp.zeros((spare, LANES), jnp.float32))
        pbuf[h, gx] = jnp.concatenate(found, axis=0)
        for d in range(1, n_gx):
            pcopy(h, (gx + d) % n_gx).start()

    def settle(h):
        whole = pbuf.at[h, pl.ds(0, n_gx - 1)]
        pltpu.make_async_copy(whole, whole, precv.at[h]).wait()
        inv = lax.rsqrt(jnp.sum(pbuf[h], axis=0) / total_cols + 1e-06)
        for r in range(tiles):
            rows = pl.ds(h * half + r * LANES, LANES)
            col = jnp.broadcast_to(inv[r:r + 1, :], (LANES, LANES)).T
            for t in range(lane_tiles):
                cols = pl.ds(t * LANES, LANES)
                o_ref[rows, cols] = o_ref[rows, cols] * col

    is_end = jnp.logical_or(z == 0, z == line - 1)
    late(line - 2, 0)
    late(line - 2, 1, is_end)
    late(line - 1, 0)
    power(0)
    late(line - 2, 1, jnp.logical_not(is_end))
    late(line - 1, 1)
    a_arrived(blk(pair, 1 - y), 1)
    unit(blk(pair, 1 - y), 1)
    power(1)

    for h in range(2):
        to_side(z, h).wait_send()
        pl.when(has_up)(lambda h=h: to_up(z, h).wait_send())
        pl.when(has_down)(lambda h=h: own_down(h).wait_send())
    for s in range(1, line):
        for h in range(2):
            @pl.when(z - s >= 0)
            def _():
                pl.when(has_up)(lambda: to_up(z - s, h).wait_send())
                if h == 0 or s > 1:
                    to_side(z - s, h).wait_send()
                else:
                    pl.when(z - s != pair)(lambda: to_side(z - s, h).wait_send())

            @pl.when(z + s < line)
            def _():
                pl.when(has_down)(lambda: to_down(z + s, h).wait_send())
                if h == 0 or s > 1:
                    to_side(z + s, h).wait_send()
                else:
                    pl.when(z + s != pair)(lambda: to_side(z + s, h).wait_send())
    to_across().wait_send()
    for c in range(nc):
        to_mate(gy * nc + c).wait_send()
        for dx in range(1, xn):
            to_x(dx, c).wait_send()
            to_mate(x_peer(dx) * nc + c).wait_send()

    for h in range(2):
        settle(h)
    for h in range(2):
        whole = pbuf.at[h, pl.ds(0, n_gx - 1)]
        pltpu.make_async_copy(whole, whole, psend.at[h]).wait()


def solution(mesh):
    n_gx, n_gy = mesh.shape["gx"], mesh.shape["gy"]

    def shards(first_factor, second_factor, result_in, pivot_scale):
        rows, ka = first_factor.shape
        kb, cols = second_factor.shape
        inner = ka * n_gx
        half, nc, line, xn = rows // 2, kb // ka, n_gx // 2, n_gy // 2
        slot = -(-(half // LANES) // 8) * 8
        held = 2 * (rows * inner + inner * cols) + 4 * rows * cols
        dma = pltpu.SemaphoreType.DMA
        hbm = pl.BlockSpec(memory_space=pltpu.HBM)
        return pl.pallas_call(
            functools.partial(kernel, n_gx, n_gy),
            out_shape=jax.ShapeDtypeStruct((rows, cols), jnp.float32),
            in_specs=[hbm] * 4,
            out_specs=pl.BlockSpec(memory_space=pltpu.VMEM),
            scratch_shapes=[
                pltpu.VMEM((n_gx, 2, half, ka), jnp.bfloat16),
                pltpu.VMEM((n_gx, ka, cols), jnp.bfloat16),
                pltpu.VMEM((2, n_gx, slot, LANES), jnp.float32),
                pltpu.VMEM((1, inner), jnp.float32),
                dma((2,)), dma((nc,)), dma, dma,
                dma((n_gx, 2)), dma((n_gx,)),
                dma((line, 2)), dma((2,)), dma((line, 2)), dma,
                dma((n_gx,)), dma((max(xn - 1, 1) * nc,)),
                dma((2,)), dma((2,)),
            ],
            compiler_params=pltpu.CompilerParams(
                collective_id=0, has_side_effects=True, vmem_limit_bytes=held + 8 * 2**20),
        )(first_factor, second_factor, result_in, pivot_scale.reshape(1, inner))

    return jax.shard_map(
        shards,
        mesh=mesh,
        in_specs=(P("gy", "gx"), P("gy", "gx"), P("gy", "gx"), P()),
        out_specs=P("gy", "gx"),
        check_vma=False,
    )
```

```python
import functools

import jax
import jax.numpy as jnp
from jax import lax
from jax.experimental import pallas as pl
from jax.experimental.pallas import tpu as pltpu
from jax.sharding import PartitionSpec as P

MESH = pl.DeviceIdType.MESH
LANES = 128
PARTS = 4


def kernel(n_gx, n_gy, a_ref, b_ref, r_ref, p_ref, o_ref, abuf, bbuf, pbuf, pv,
           a_loc, b_loc, r_loc, p_loc, arecv, brecv, zs, zd, ys, xs, bcs, bxs, psend, precv):
    part, ka = abuf.shape[2], abuf.shape[3]
    nc = b_ref.shape[0] // ka
    line, xn = n_gx // 2, n_gy // 2
    gx, gy = lax.axis_index("gx"), lax.axis_index("gy")
    z, y = gx // 2, gx % 2
    x, core = gy // 2, gy % 2
    pair = z + 1 - 2 * (z % 2)
    total_cols = o_ref.shape[1] * n_gx

    def blk(zz, yy):
        return zz * 2 + yy

    up = {"gx": blk(jnp.minimum(z + 1, line - 1), y), "gy": gy}
    down = {"gx": blk(jnp.maximum(z - 1, 0), y), "gy": gy}
    side = {"gx": blk(z, 1 - y), "gy": gy}
    across = {"gx": blk(pair, y), "gy": gy}
    mate = {"gx": gx, "gy": x * 2 + 1 - core}

    def x_peer(dx):
        return ((x + dx) % xn) * 2 + core

    a_in = [pltpu.make_async_copy(a_ref.at[pl.ds(h * part, part)], abuf.at[gx, h], a_loc.at[h]) for h in range(PARTS)]
    b_in = [pltpu.make_async_copy(b_ref.at[pl.ds(c * ka, ka)], bbuf.at[gy * nc + c], b_loc.at[c]) for c in range(nc)]
    p_in = pltpu.make_async_copy(p_ref, pv, p_loc)
    r_in = pltpu.make_async_copy(r_ref, o_ref, r_loc)
    for cp in a_in + b_in + [p_in, r_in]:
        cp.start()

    barrier = pltpu.get_barrier_semaphore()
    for d in range(1, n_gx):
        pl.semaphore_signal(barrier, inc=1, device_id={"gx": (gx + d) % n_gx, "gy": gy}, device_id_type=MESH)
    pl.semaphore_signal(barrier, inc=1, device_id=mate, device_id_type=MESH)
    for dx in range(1, xn):
        pl.semaphore_signal(barrier, inc=1, device_id={"gx": gx, "gy": x_peer(dx)}, device_id_type=MESH)
    pl.semaphore_wait(barrier, n_gx - 1 + 1 + xn - 1)

    def acopy(j, h, sem, dev):
        return pltpu.make_async_remote_copy(
            src_ref=abuf.at[j, h], dst_ref=abuf.at[j, h], send_sem=sem,
            recv_sem=arecv.at[j, h], device_id=dev, device_id_type=MESH)

    def bcopy(j, sem, dev):
        return pltpu.make_async_remote_copy(
            src_ref=bbuf.at[j], dst_ref=bbuf.at[j], send_sem=sem,
            recv_sem=brecv.at[j], device_id=dev, device_id_type=MESH)

    def a_arrived(j, h):
        acopy(j, h, xs.at[0], side).wait_recv()

    def b_arrived(j):
        bcopy(j, xs.at[0], mate).wait_recv()

    def to_side(zz, h):
        return acopy(blk(zz, y), h, ys.at[zz, h], side)

    def to_up(zz, h):
        return acopy(blk(zz, y), h, zs.at[zz, h], up)

    def to_down(zz, h):
        return acopy(blk(zz, y), h, zs.at[zz, h], down)

    def own_down(h):
        return acopy(gx, h, zd.at[h], down)

    def to_across(h):
        return acopy(blk(z, 1 - y), h, xs.at[h], across)

    def to_mate(j):
        return bcopy(j, bcs.at[j], mate)

    def to_x(dx, c):
        return bcopy(gy * nc + c, bxs.at[(dx - 1) * nc + c], {"gx": gx, "gy": x_peer(dx)})

    has_up, has_down = z + 1 < line, z > 0

    for h in range(PARTS):
        a_in[h].wait()
        to_side(z, h).start()
        pl.when(has_up)(lambda h=h: to_up(z, h).start())
        pl.when(has_down)(lambda h=h: own_down(h).start())
    for c in range(nc):
        b_in[c].wait()
        for dx in range(1, xn):
            to_x(dx, c).start()
        to_mate(gy * nc + c).start()

    def z_round(s, h):
        @pl.when(z - s >= 0)
        def _():
            zz = z - s
            a_arrived(blk(zz, y), h)
            pl.when(has_up)(lambda: to_up(zz, h).start())
            if h < PARTS // 2 or s > 1:
                to_side(zz, h).start()
            else:
                pl.when(zz != pair)(lambda: to_side(zz, h).start())

        @pl.when(z + s < line)
        def _():
            zz = z + s
            a_arrived(blk(zz, y), h)
            pl.when(has_down)(lambda: to_down(zz, h).start())
            if h < PARTS // 2 or s > 1:
                to_side(zz, h).start()
            else:
                pl.when(zz != pair)(lambda: to_side(zz, h).start())

    def side_wait(zz, h, s):
        if h < PARTS // 2 or s != 1:
            a_arrived(blk(zz, 1 - y), h)
        else:
            pl.when(zz != pair)(lambda: a_arrived(blk(zz, 1 - y), h))

    def y_round(s):
        for h in range(PARTS):
            if s == 0:
                side_wait(z, h, s)
            else:
                pl.when(z - s >= 0)(lambda h=h: side_wait(z - s, h, s))
                pl.when(z + s < line)(lambda h=h: side_wait(z + s, h, s))

    def b_round(c):
        for dx in range(1, xn):
            j = x_peer(dx) * nc + c
            b_arrived(j)
            to_mate(j).start()

    def unit(j, h, n):
        rows = pl.ds(pl.multiple_of(h * part, part), n * part)
        scale = pv[:, pl.ds(pl.multiple_of(j * ka, ka), ka)]
        left = abuf[j, pl.ds(h, n)].reshape(n * part, ka).astype(jnp.float32)
        left = (left * scale).astype(jnp.bfloat16)
        o_ref[rows, :] = o_ref[rows, :] - jnp.dot(left, bbuf[j], preferred_element_type=jnp.float32)

    def compute(yy, pred, first=0, steps=2):
        def body(t, carry):
            zz, h = t // steps, first + t % steps
            pl.when(pred(zz, h))(lambda: unit(blk(zz, yy), h * (PARTS // 2), PARTS // 2))
            return carry
        lax.fori_loop(0, steps * line, body, 0)

    def near(zz, s):
        return jnp.logical_and(zz - z <= s, z - zz <= s)

    for s in range(1, line - 1):
        if s >= 2:
            y_round(s - 2)
        for h in range(PARTS):
            z_round(s, h)
        if s - 1 < nc:
            b_round(s - 1)
    for c in range(line - 2, nc):
        b_round(c)
    for h in range(PARTS // 2, PARTS):
        to_across(h).start()
    for c in range(nc):
        b_arrived(mate["gy"] * nc + c)
        for dx in range(1, xn):
            b_arrived((((x + dx) % xn) * 2 + 1 - core) * nc + c)
    p_in.wait()
    r_in.wait()

    z_round(line - 1, 0)
    compute(y, lambda zz, h: near(zz, line - 2), 0, 1)
    z_round(line - 1, 1)
    compute(y, lambda zz, h: near(zz, line - 2), 1, 1)
    z_round(line - 1, 2)
    y_round(line - 3)
    compute(1 - y, lambda zz, h: jnp.logical_and(near(zz, line - 3), jnp.logical_or(zz != pair, h == 0)))
    z_round(line - 1, 3)
    compute(y, lambda zz, h: jnp.logical_not(near(zz, line - 2)))

    is_end = jnp.logical_or(z == 0, z == line - 1)

    def late(s, h, n, when=True):
        zz = jnp.where(z >= s, z - s, z + s)

        @pl.when(jnp.logical_and(jnp.logical_or(z >= s, z + s < line), when))
        def _():
            for i in range(n):
                a_arrived(blk(zz, 1 - y), h + i)
            unit(blk(zz, 1 - y), h, n)

    tiles = part // LANES
    lane_tiles = o_ref.shape[1] // LANES

    def pcopy(h, peer):
        return pltpu.make_async_remote_copy(
            src_ref=pbuf.at[h, gx], dst_ref=pbuf.at[h, gx], send_sem=psend.at[h],
            recv_sem=precv.at[h], device_id={"gx": peer, "gy": gy}, device_id_type=MESH)

    def power(h):
        found = []
        for r in range(tiles):
            block = o_ref[pl.ds(h * part + r * LANES, LANES), :]
            acc = jnp.zeros((LANES, LANES), jnp.float32)
            for t in range(lane_tiles):
                piece = block[:, t * LANES:(t + 1) * LANES]
                acc = acc + piece * piece
            found.append(jnp.sum(acc.T, axis=0, keepdims=True))
        spare = pbuf.shape[2] - tiles
        if spare:
            found.append(jnp.zeros((spare, LANES), jnp.float32))
        pbuf[h, gx] = jnp.concatenate(found, axis=0)
        for d in range(1, n_gx):
            pcopy(h, (gx + d) % n_gx).start()

    def settle(h):
        whole = pbuf.at[h, pl.ds(0, n_gx - 1)]
        pltpu.make_async_copy(whole, whole, precv.at[h]).wait()
        inv = lax.rsqrt(jnp.sum(pbuf[h], axis=0) / total_cols + 1e-06)
        for r in range(tiles):
            rows = pl.ds(h * part + r * LANES, LANES)
            col = jnp.broadcast_to(inv[r:r + 1, :], (LANES, LANES)).T
            for t in range(lane_tiles):
                cols = pl.ds(t * LANES, LANES)
                o_ref[rows, cols] = o_ref[rows, cols] * col

    for h in range(0, PARTS, PARTS // 2):
        late(line - 2, h, PARTS // 2, is_end)
    for h in range(PARTS):
        late(jnp.where(is_end, line - 1, line - 2), h, 1)
        if h >= PARTS // 2:
            a_arrived(blk(pair, 1 - y), h)
            unit(blk(pair, 1 - y), h, 1)
        power(h)

    for h in range(PARTS):
        settle(h)

    for h in range(PARTS):
        to_side(z, h).wait_send()
        pl.when(has_up)(lambda h=h: to_up(z, h).wait_send())
        pl.when(has_down)(lambda h=h: own_down(h).wait_send())
    for s in range(1, line):
        for h in range(PARTS):
            @pl.when(z - s >= 0)
            def _():
                pl.when(has_up)(lambda: to_up(z - s, h).wait_send())
                if h < PARTS // 2 or s > 1:
                    to_side(z - s, h).wait_send()
                else:
                    pl.when(z - s != pair)(lambda: to_side(z - s, h).wait_send())

            @pl.when(z + s < line)
            def _():
                pl.when(has_down)(lambda: to_down(z + s, h).wait_send())
                if h < PARTS // 2 or s > 1:
                    to_side(z + s, h).wait_send()
                else:
                    pl.when(z + s != pair)(lambda: to_side(z + s, h).wait_send())
    for h in range(PARTS // 2, PARTS):
        to_across(h).wait_send()
    for c in range(nc):
        to_mate(gy * nc + c).wait_send()
        for dx in range(1, xn):
            to_x(dx, c).wait_send()
            to_mate(x_peer(dx) * nc + c).wait_send()

    for h in range(PARTS):
        whole = pbuf.at[h, pl.ds(0, n_gx - 1)]
        pltpu.make_async_copy(whole, whole, psend.at[h]).wait()


def solution(mesh):
    n_gx, n_gy = mesh.shape["gx"], mesh.shape["gy"]

    def shards(first_factor, second_factor, result_in, pivot_scale):
        rows, ka = first_factor.shape
        kb, cols = second_factor.shape
        inner = ka * n_gx
        part, nc, line, xn = rows // PARTS, kb // ka, n_gx // 2, n_gy // 2
        slot = -(-(part // LANES) // 8) * 8
        held = 2 * (rows * inner + inner * cols) + 4 * rows * cols
        dma = pltpu.SemaphoreType.DMA
        hbm = pl.BlockSpec(memory_space=pltpu.HBM)
        return pl.pallas_call(
            functools.partial(kernel, n_gx, n_gy),
            out_shape=jax.ShapeDtypeStruct((rows, cols), jnp.float32),
            in_specs=[hbm] * 4,
            out_specs=pl.BlockSpec(memory_space=pltpu.VMEM),
            scratch_shapes=[
                pltpu.VMEM((n_gx, PARTS, part, ka), jnp.bfloat16),
                pltpu.VMEM((n_gx, ka, cols), jnp.bfloat16),
                pltpu.VMEM((PARTS, n_gx, slot, LANES), jnp.float32),
                pltpu.VMEM((1, inner), jnp.float32),
                dma((PARTS,)), dma((nc,)), dma, dma,
                dma((n_gx, PARTS)), dma((n_gx,)),
                dma((line, PARTS)), dma((PARTS,)), dma((line, PARTS)), dma((PARTS,)),
                dma((n_gx,)), dma((max(xn - 1, 1) * nc,)),
                dma((PARTS,)), dma((PARTS,)),
            ],
            compiler_params=pltpu.CompilerParams(
                collective_id=0, has_side_effects=True, vmem_limit_bytes=held + 8 * 2**20),
        )(*[pltpu.with_memory_space_constraint(v, pltpu.HBM) for v in (first_factor, second_factor, result_in, pivot_scale.reshape(1, inner))])

    return jax.shard_map(
        shards,
        mesh=mesh,
        in_specs=(P("gy", "gx"), P("gy", "gx"), P("gy", "gx"), P()),
        out_specs=P("gy", "gx"),
        check_vma=False,
    )
```

```python
import functools

import jax
import jax.numpy as jnp
from jax import lax
from jax.experimental import pallas as pl
from jax.experimental.pallas import tpu as pltpu
from jax.sharding import PartitionSpec as P

MESH = pl.DeviceIdType.MESH
LANES = 128
PARTS = 4


def kernel(n_gx, n_gy, a_ref, b_ref, r_ref, p_ref, o_ref, abuf, bbuf, pbuf, pv,
           a_loc, b_loc, r_loc, p_loc, arecv, brecv, zs, zd, ys, xs, bcs, bxs, psend, precv):
    part, ka = abuf.shape[2], abuf.shape[3]
    nc = b_ref.shape[0] // ka
    line, xn = n_gx // 2, n_gy // 2
    gx, gy = lax.axis_index("gx"), lax.axis_index("gy")
    z, y = gx // 2, gx % 2
    x, core = gy // 2, gy % 2
    pair = z + 1 - 2 * (z % 2)
    total_cols = o_ref.shape[1] * n_gx

    def blk(zz, yy):
        return zz * 2 + yy

    up = {"gx": blk(jnp.minimum(z + 1, line - 1), y), "gy": gy}
    down = {"gx": blk(jnp.maximum(z - 1, 0), y), "gy": gy}
    side = {"gx": blk(z, 1 - y), "gy": gy}
    across = {"gx": blk(pair, y), "gy": gy}
    mate = {"gx": gx, "gy": x * 2 + 1 - core}

    def x_peer(dx):
        return ((x + dx) % xn) * 2 + core

    has_up, has_down = z + 1 < line, z > 0
    barrier = pltpu.get_barrier_semaphore()

    def greet(dev):
        pl.semaphore_signal(barrier, inc=1, device_id=dev, device_id_type=MESH)

    pl.when(has_up)(lambda: greet(up))
    pl.when(has_down)(lambda: greet(down))
    greet(side)
    for dx in range(1, xn):
        greet({"gx": gx, "gy": x_peer(dx)})
    greet(mate)

    a_in = [pltpu.make_async_copy(a_ref.at[pl.ds(h * part, part)], abuf.at[gx, h], a_loc.at[h]) for h in range(PARTS)]
    b_in = [pltpu.make_async_copy(b_ref.at[pl.ds(c * ka, ka)], bbuf.at[gy * nc + c], b_loc.at[c]) for c in range(nc)]
    p_in = pltpu.make_async_copy(p_ref, pv, p_loc)
    r_in = pltpu.make_async_copy(r_ref, o_ref, r_loc)
    for cp in a_in + b_in + [p_in, r_in]:
        cp.start()

    pl.semaphore_wait(barrier, 2 + xn - 1 + has_up.astype(jnp.int32) + has_down.astype(jnp.int32))

    def acopy(j, h, sem, dev):
        return pltpu.make_async_remote_copy(
            src_ref=abuf.at[j, h], dst_ref=abuf.at[j, h], send_sem=sem,
            recv_sem=arecv.at[j, h], device_id=dev, device_id_type=MESH)

    def bcopy(j, sem, dev):
        return pltpu.make_async_remote_copy(
            src_ref=bbuf.at[j], dst_ref=bbuf.at[j], send_sem=sem,
            recv_sem=brecv.at[j], device_id=dev, device_id_type=MESH)

    def a_arrived(j, h):
        acopy(j, h, xs.at[0], side).wait_recv()

    def b_arrived(j):
        bcopy(j, xs.at[0], mate).wait_recv()

    def to_side(zz, h):
        return acopy(blk(zz, y), h, ys.at[zz, h], side)

    def to_up(zz, h):
        return acopy(blk(zz, y), h, zs.at[zz, h], up)

    def to_down(zz, h):
        return acopy(blk(zz, y), h, zs.at[zz, h], down)

    def own_down(h):
        return acopy(gx, h, zd.at[h], down)

    def to_across(h):
        return acopy(blk(z, 1 - y), h, xs.at[h], across)

    def to_mate(j):
        return bcopy(j, bcs.at[j], mate)

    def to_x(dx, c):
        return bcopy(gy * nc + c, bxs.at[(dx - 1) * nc + c], {"gx": gx, "gy": x_peer(dx)})

    for h in range(PARTS):
        a_in[h].wait()
        to_side(z, h).start()
        pl.when(has_up)(lambda h=h: to_up(z, h).start())
        pl.when(has_down)(lambda h=h: own_down(h).start())
    for c in range(nc):
        b_in[c].wait()
        for dx in range(1, xn):
            to_x(dx, c).start()
        to_mate(gy * nc + c).start()

    def z_round(s, h):
        @pl.when(z - s >= 0)
        def _():
            zz = z - s
            a_arrived(blk(zz, y), h)
            pl.when(has_up)(lambda: to_up(zz, h).start())
            if h < PARTS // 2 or s > 1:
                to_side(zz, h).start()
            else:
                pl.when(zz != pair)(lambda: to_side(zz, h).start())

        @pl.when(z + s < line)
        def _():
            zz = z + s
            a_arrived(blk(zz, y), h)
            pl.when(has_down)(lambda: to_down(zz, h).start())
            if h < PARTS // 2 or s > 1:
                to_side(zz, h).start()
            else:
                pl.when(zz != pair)(lambda: to_side(zz, h).start())

    def side_wait(zz, h, s):
        if h < PARTS // 2 or s != 1:
            a_arrived(blk(zz, 1 - y), h)
        else:
            pl.when(zz != pair)(lambda: a_arrived(blk(zz, 1 - y), h))

    def y_round(s):
        for h in range(PARTS):
            if s == 0:
                side_wait(z, h, s)
            else:
                pl.when(z - s >= 0)(lambda h=h: side_wait(z - s, h, s))
                pl.when(z + s < line)(lambda h=h: side_wait(z + s, h, s))

    def b_round(c):
        for dx in range(1, xn):
            j = x_peer(dx) * nc + c
            b_arrived(j)
            to_mate(j).start()

    def unit(j, h, n):
        rows = pl.ds(pl.multiple_of(h * part, part), n * part)
        scale = pv[:, pl.ds(pl.multiple_of(j * ka, ka), ka)]
        left = abuf[j, pl.ds(h, n)].reshape(n * part, ka).astype(jnp.float32)
        left = (left * scale).astype(jnp.bfloat16)
        o_ref[rows, :] = o_ref[rows, :] - jnp.dot(left, bbuf[j], preferred_element_type=jnp.float32)

    def compute(yy, pred, first=0, steps=2):
        def body(t, carry):
            zz, h = t // steps, first + t % steps
            pl.when(pred(zz, h))(lambda: unit(blk(zz, yy), h * (PARTS // 2), PARTS // 2))
            return carry
        lax.fori_loop(0, steps * line, body, 0)

    def near(zz, s):
        return jnp.logical_and(zz - z <= s, z - zz <= s)

    for s in range(1, line - 1):
        if s >= 2:
            y_round(s - 2)
        for h in range(PARTS):
            z_round(s, h)
        if s - 1 < nc:
            b_round(s - 1)
    for c in range(line - 2, nc):
        b_round(c)
    for h in range(PARTS // 2, PARTS):
        to_across(h).start()
    for c in range(nc):
        b_arrived(mate["gy"] * nc + c)
        for dx in range(1, xn):
            b_arrived((((x + dx) % xn) * 2 + 1 - core) * nc + c)
    p_in.wait()
    r_in.wait()

    z_round(line - 1, 0)
    compute(y, lambda zz, h: near(zz, line - 2), 0, 1)
    z_round(line - 1, 1)
    compute(y, lambda zz, h: near(zz, line - 2), 1, 1)
    z_round(line - 1, 2)
    y_round(line - 3)
    compute(1 - y, lambda zz, h: jnp.logical_and(near(zz, line - 3), jnp.logical_or(zz != pair, h == 0)))
    z_round(line - 1, 3)
    compute(y, lambda zz, h: jnp.logical_not(near(zz, line - 2)))

    is_end = jnp.logical_or(z == 0, z == line - 1)

    def late(s, h, n, when=True):
        zz = jnp.where(z >= s, z - s, z + s)

        @pl.when(jnp.logical_and(jnp.logical_or(z >= s, z + s < line), when))
        def _():
            for i in range(n):
                a_arrived(blk(zz, 1 - y), h + i)
            unit(blk(zz, 1 - y), h, n)

    tiles = part // LANES
    lane_tiles = o_ref.shape[1] // LANES

    def pcopy(h, peer):
        return pltpu.make_async_remote_copy(
            src_ref=pbuf.at[h, gx], dst_ref=pbuf.at[h, gx], send_sem=psend.at[h],
            recv_sem=precv.at[h], device_id={"gx": peer, "gy": gy}, device_id_type=MESH)

    def power(h):
        found = []
        for r in range(tiles):
            block = o_ref[pl.ds(h * part + r * LANES, LANES), :]
            acc = jnp.zeros((LANES, LANES), jnp.float32)
            for t in range(lane_tiles):
                piece = block[:, t * LANES:(t + 1) * LANES]
                acc = acc + piece * piece
            found.append(jnp.sum(acc.T, axis=0, keepdims=True))
        spare = pbuf.shape[2] - tiles
        if spare:
            found.append(jnp.zeros((spare, LANES), jnp.float32))
        pbuf[h, gx] = jnp.concatenate(found, axis=0)
        for d in range(1, n_gx):
            pcopy(h, (gx + d) % n_gx).start()

    def settle(h):
        whole = pbuf.at[h, pl.ds(0, n_gx - 1)]
        pltpu.make_async_copy(whole, whole, precv.at[h]).wait()
        inv = lax.rsqrt(jnp.sum(pbuf[h], axis=0) / total_cols + 1e-06)
        for r in range(tiles):
            rows = pl.ds(h * part + r * LANES, LANES)
            col = jnp.broadcast_to(inv[r:r + 1, :], (LANES, LANES)).T
            for t in range(lane_tiles):
                cols = pl.ds(t * LANES, LANES)
                o_ref[rows, cols] = o_ref[rows, cols] * col

    for h in range(0, PARTS, PARTS // 2):
        late(line - 2, h, PARTS // 2, is_end)
    for h in range(PARTS):
        late(jnp.where(is_end, line - 1, line - 2), h, 1)
        if h >= PARTS // 2:
            a_arrived(blk(pair, 1 - y), h)
            unit(blk(pair, 1 - y), h, 1)
        power(h)

    for h in range(PARTS):
        settle(h)

    for h in range(PARTS):
        to_side(z, h).wait_send()
        pl.when(has_up)(lambda h=h: to_up(z, h).wait_send())
        pl.when(has_down)(lambda h=h: own_down(h).wait_send())
    for s in range(1, line):
        for h in range(PARTS):
            @pl.when(z - s >= 0)
            def _():
                pl.when(has_up)(lambda: to_up(z - s, h).wait_send())
                if h < PARTS // 2 or s > 1:
                    to_side(z - s, h).wait_send()
                else:
                    pl.when(z - s != pair)(lambda: to_side(z - s, h).wait_send())

            @pl.when(z + s < line)
            def _():
                pl.when(has_down)(lambda: to_down(z + s, h).wait_send())
                if h < PARTS // 2 or s > 1:
                    to_side(z + s, h).wait_send()
                else:
                    pl.when(z + s != pair)(lambda: to_side(z + s, h).wait_send())
    for h in range(PARTS // 2, PARTS):
        to_across(h).wait_send()
    for c in range(nc):
        to_mate(gy * nc + c).wait_send()
        for dx in range(1, xn):
            to_x(dx, c).wait_send()
            to_mate(x_peer(dx) * nc + c).wait_send()

    for h in range(PARTS):
        whole = pbuf.at[h, pl.ds(0, n_gx - 1)]
        pltpu.make_async_copy(whole, whole, psend.at[h]).wait()


def solution(mesh):
    n_gx, n_gy = mesh.shape["gx"], mesh.shape["gy"]

    def shards(first_factor, second_factor, result_in, pivot_scale):
        rows, ka = first_factor.shape
        kb, cols = second_factor.shape
        inner = ka * n_gx
        part, nc, line, xn = rows // PARTS, kb // ka, n_gx // 2, n_gy // 2
        slot = -(-(part // LANES) // 8) * 8
        held = 2 * (rows * inner + inner * cols) + 4 * rows * cols
        dma = pltpu.SemaphoreType.DMA
        hbm = pl.BlockSpec(memory_space=pltpu.HBM)
        return pl.pallas_call(
            functools.partial(kernel, n_gx, n_gy),
            out_shape=jax.ShapeDtypeStruct((rows, cols), jnp.float32),
            in_specs=[hbm] * 4,
            out_specs=pl.BlockSpec(memory_space=pltpu.VMEM),
            scratch_shapes=[
                pltpu.VMEM((n_gx, PARTS, part, ka), jnp.bfloat16),
                pltpu.VMEM((n_gx, ka, cols), jnp.bfloat16),
                pltpu.VMEM((PARTS, n_gx, slot, LANES), jnp.float32),
                pltpu.VMEM((1, inner), jnp.float32),
                dma((PARTS,)), dma((nc,)), dma, dma,
                dma((n_gx, PARTS)), dma((n_gx,)),
                dma((line, PARTS)), dma((PARTS,)), dma((line, PARTS)), dma((PARTS,)),
                dma((n_gx,)), dma((max(xn - 1, 1) * nc,)),
                dma((PARTS,)), dma((PARTS,)),
            ],
            compiler_params=pltpu.CompilerParams(
                collective_id=0, has_side_effects=True, vmem_limit_bytes=held + 8 * 2**20),
        )(*[pltpu.with_memory_space_constraint(v, pltpu.HBM) for v in (first_factor, second_factor, result_in, pivot_scale.reshape(1, inner))])

    return jax.shard_map(
        shards,
        mesh=mesh,
        in_specs=(P("gy", "gx"), P("gy", "gx"), P("gy", "gx"), P()),
        out_specs=P("gy", "gx"),
        check_vma=False,
    )
```

```python
import functools

import jax
import jax.numpy as jnp
from jax import lax
from jax.experimental import pallas as pl
from jax.experimental.pallas import tpu as pltpu
from jax.sharding import PartitionSpec as P

MESH = pl.DeviceIdType.MESH
LANES = 128
PARTS = 4


def kernel(n_gx, n_gy, a_ref, b_ref, r_ref, p_ref, o_ref, abuf, bbuf, pbuf, pv,
           a_loc, b_loc, r_loc, p_loc, arecv, brecv, zs, zd, ys, xs, bcs, bxs, psend, precv):
    part, ka = abuf.shape[2], abuf.shape[3]
    nc = b_ref.shape[0] // ka
    line, xn = n_gx // 2, n_gy // 2
    gx, gy = lax.axis_index("gx"), lax.axis_index("gy")
    z, y = gx // 2, gx % 2
    x, core = gy // 2, gy % 2
    pair = z + 1 - 2 * (z % 2)
    total_cols = o_ref.shape[1] * n_gx

    def blk(zz, yy):
        return zz * 2 + yy

    up = {"gx": blk(jnp.minimum(z + 1, line - 1), y), "gy": gy}
    down = {"gx": blk(jnp.maximum(z - 1, 0), y), "gy": gy}
    side = {"gx": blk(z, 1 - y), "gy": gy}
    across = {"gx": blk(pair, y), "gy": gy}
    mate = {"gx": gx, "gy": x * 2 + 1 - core}

    def x_peer(dx):
        return ((x + dx) % xn) * 2 + core

    has_up, has_down = z + 1 < line, z > 0
    barrier = pltpu.get_barrier_semaphore()

    def greet(dev):
        pl.semaphore_signal(barrier, inc=1, device_id=dev, device_id_type=MESH)

    pl.when(has_up)(lambda: greet(up))
    pl.when(has_down)(lambda: greet(down))
    greet(side)
    for dx in range(1, xn):
        greet({"gx": gx, "gy": x_peer(dx)})
    greet(mate)

    a_in = [pltpu.make_async_copy(a_ref.at[pl.ds(h * part, part)], abuf.at[gx, h], a_loc.at[h]) for h in range(PARTS)]
    b_in = [pltpu.make_async_copy(b_ref.at[pl.ds(c * ka, ka)], bbuf.at[gy * nc + c], b_loc.at[c]) for c in range(nc)]
    p_in = pltpu.make_async_copy(p_ref, pv, p_loc)
    r_in = pltpu.make_async_copy(r_ref, o_ref, r_loc)
    for cp in a_in + b_in + [p_in, r_in]:
        cp.start()

    pl.semaphore_wait(barrier, 2 + xn - 1 + has_up.astype(jnp.int32) + has_down.astype(jnp.int32))

    def acopy(j, h, sem, dev):
        return pltpu.make_async_remote_copy(
            src_ref=abuf.at[j, h], dst_ref=abuf.at[j, h], send_sem=sem,
            recv_sem=arecv.at[j, h], device_id=dev, device_id_type=MESH)

    def bcopy(j, sem, dev):
        return pltpu.make_async_remote_copy(
            src_ref=bbuf.at[j], dst_ref=bbuf.at[j], send_sem=sem,
            recv_sem=brecv.at[j], device_id=dev, device_id_type=MESH)

    def a_arrived(j, h):
        acopy(j, h, xs.at[0], side).wait_recv()

    def b_arrived(j):
        bcopy(j, xs.at[0], mate).wait_recv()

    def to_side(zz, h):
        return acopy(blk(zz, y), h, ys.at[zz, h], side)

    def to_up(zz, h):
        return acopy(blk(zz, y), h, zs.at[zz, h], up)

    def to_down(zz, h):
        return acopy(blk(zz, y), h, zs.at[zz, h], down)

    def own_down(h):
        return acopy(gx, h, zd.at[h], down)

    def to_across(h):
        return acopy(blk(z, 1 - y), h, xs.at[h], across)

    def to_mate(j):
        return bcopy(j, bcs.at[j], mate)

    def to_x(dx, c):
        return bcopy(gy * nc + c, bxs.at[(dx - 1) * nc + c], {"gx": gx, "gy": x_peer(dx)})

    for h in range(PARTS):
        a_in[h].wait()
        to_side(z, h).start()
        pl.when(has_up)(lambda h=h: to_up(z, h).start())
        pl.when(has_down)(lambda h=h: own_down(h).start())
    for c in range(nc):
        b_in[c].wait()
    for i in range(nc):
        c = (i + y) % nc
        for dx in range(1, xn):
            to_x(dx, c).start()
        to_mate(gy * nc + c).start()

    def z_round(s, h):
        @pl.when(z - s >= 0)
        def _():
            zz = z - s
            a_arrived(blk(zz, y), h)
            pl.when(has_up)(lambda: to_up(zz, h).start())
            if h < PARTS // 2 or s > 1:
                to_side(zz, h).start()
            else:
                pl.when(zz != pair)(lambda: to_side(zz, h).start())

        @pl.when(z + s < line)
        def _():
            zz = z + s
            a_arrived(blk(zz, y), h)
            pl.when(has_down)(lambda: to_down(zz, h).start())
            if h < PARTS // 2 or s > 1:
                to_side(zz, h).start()
            else:
                pl.when(zz != pair)(lambda: to_side(zz, h).start())

    def side_wait(zz, h, s):
        if h < PARTS // 2 or s != 1:
            a_arrived(blk(zz, 1 - y), h)
        else:
            pl.when(zz != pair)(lambda: a_arrived(blk(zz, 1 - y), h))

    def y_round(s):
        for h in range(PARTS):
            if s == 0:
                side_wait(z, h, s)
            else:
                pl.when(z - s >= 0)(lambda h=h: side_wait(z - s, h, s))
                pl.when(z + s < line)(lambda h=h: side_wait(z + s, h, s))

    def b_round(i):
        c = (i + y) % nc
        for dx in range(1, xn):
            j = x_peer(dx) * nc + c
            b_arrived(j)
            to_mate(j).start()

    def unit(j, h, n):
        rows = pl.ds(pl.multiple_of(h * part, part), n * part)
        scale = pv[:, pl.ds(pl.multiple_of(j * ka, ka), ka)]
        left = abuf[j, pl.ds(h, n)].reshape(n * part, ka).astype(jnp.float32)
        left = (left * scale).astype(jnp.bfloat16)
        o_ref[rows, :] = o_ref[rows, :] - jnp.dot(left, bbuf[j], preferred_element_type=jnp.float32)

    def compute(yy, pred, first=0, steps=2):
        def body(t, carry):
            zz, h = t // steps, first + t % steps
            pl.when(pred(zz, h))(lambda: unit(blk(zz, yy), h * (PARTS // 2), PARTS // 2))
            return carry
        lax.fori_loop(0, steps * line, body, 0)

    def near(zz, s):
        return jnp.logical_and(zz - z <= s, z - zz <= s)

    def b_settled(i):
        c = (i + y) % nc
        b_arrived(mate["gy"] * nc + c)
        for dx in range(1, xn):
            b_arrived((((x + dx) % xn) * 2 + 1 - core) * nc + c)

    early = nc == 2

    def rest(zz):
        return jnp.logical_and(near(zz, line - 2), jnp.logical_not(near(zz, 1))) if early else near(zz, line - 2)

    for s in range(1, line - 1):
        if s >= 2:
            y_round(s - 2)
        for h in range(PARTS):
            z_round(s, h)
        if s - 1 < nc:
            b_round(s - 1)
        if s == 1 and early:
            b_settled(0)
            p_in.wait()
            r_in.wait()
            compute(y, lambda zz, h: near(zz, 1))
    for c in range(line - 2, nc):
        b_round(c)
    for h in range(PARTS // 2, PARTS):
        to_across(h).start()
    for i in range(1 if early else 0, nc):
        b_settled(i)
    if not early:
        p_in.wait()
        r_in.wait()

    z_round(line - 1, 0)
    compute(y, lambda zz, h: rest(zz), 0, 1)
    z_round(line - 1, 1)
    compute(y, lambda zz, h: rest(zz), 1, 1)
    z_round(line - 1, 2)
    y_round(line - 3)
    compute(1 - y, lambda zz, h: jnp.logical_and(near(zz, line - 3), jnp.logical_or(zz != pair, h == 0)))
    z_round(line - 1, 3)
    compute(y, lambda zz, h: jnp.logical_not(near(zz, line - 2)))

    is_end = jnp.logical_or(z == 0, z == line - 1)

    def late(s, h, n, when=True):
        zz = jnp.where(z >= s, z - s, z + s)

        @pl.when(jnp.logical_and(jnp.logical_or(z >= s, z + s < line), when))
        def _():
            for i in range(n):
                a_arrived(blk(zz, 1 - y), h + i)
            unit(blk(zz, 1 - y), h, n)

    tiles = part // LANES
    lane_tiles = o_ref.shape[1] // LANES

    def pcopy(h, peer):
        return pltpu.make_async_remote_copy(
            src_ref=pbuf.at[h, gx], dst_ref=pbuf.at[h, gx], send_sem=psend.at[h],
            recv_sem=precv.at[h], device_id={"gx": peer, "gy": gy}, device_id_type=MESH)

    def power(h):
        found = []
        for r in range(tiles):
            block = o_ref[pl.ds(h * part + r * LANES, LANES), :]
            acc = jnp.zeros((LANES, LANES), jnp.float32)
            for t in range(lane_tiles):
                piece = block[:, t * LANES:(t + 1) * LANES]
                acc = acc + piece * piece
            found.append(jnp.sum(acc.T, axis=0, keepdims=True))
        spare = pbuf.shape[2] - tiles
        if spare:
            found.append(jnp.zeros((spare, LANES), jnp.float32))
        pbuf[h, gx] = jnp.concatenate(found, axis=0)
        for d in range(1, n_gx):
            pcopy(h, (gx + d) % n_gx).start()

    def settle(h):
        whole = pbuf.at[h, pl.ds(0, n_gx - 1)]
        pltpu.make_async_copy(whole, whole, precv.at[h]).wait()
        inv = lax.rsqrt(jnp.sum(pbuf[h], axis=0) / total_cols + 1e-06)
        for r in range(tiles):
            rows = pl.ds(h * part + r * LANES, LANES)
            col = jnp.broadcast_to(inv[r:r + 1, :], (LANES, LANES)).T
            for t in range(lane_tiles):
                cols = pl.ds(t * LANES, LANES)
                o_ref[rows, cols] = o_ref[rows, cols] * col

    for h in range(0, PARTS, PARTS // 2):
        late(line - 2, h, PARTS // 2, is_end)
    for h in range(PARTS):
        late(jnp.where(is_end, line - 1, line - 2), h, 1)
        if h >= PARTS // 2:
            a_arrived(blk(pair, 1 - y), h)
            unit(blk(pair, 1 - y), h, 1)
        power(h)

    for h in range(PARTS):
        settle(h)

    for h in range(PARTS):
        to_side(z, h).wait_send()
        pl.when(has_up)(lambda h=h: to_up(z, h).wait_send())
        pl.when(has_down)(lambda h=h: own_down(h).wait_send())
    for s in range(1, line):
        for h in range(PARTS):
            @pl.when(z - s >= 0)
            def _():
                pl.when(has_up)(lambda: to_up(z - s, h).wait_send())
                if h < PARTS // 2 or s > 1:
                    to_side(z - s, h).wait_send()
                else:
                    pl.when(z - s != pair)(lambda: to_side(z - s, h).wait_send())

            @pl.when(z + s < line)
            def _():
                pl.when(has_down)(lambda: to_down(z + s, h).wait_send())
                if h < PARTS // 2 or s > 1:
                    to_side(z + s, h).wait_send()
                else:
                    pl.when(z + s != pair)(lambda: to_side(z + s, h).wait_send())
    for h in range(PARTS // 2, PARTS):
        to_across(h).wait_send()
    for c in range(nc):
        to_mate(gy * nc + c).wait_send()
        for dx in range(1, xn):
            to_x(dx, c).wait_send()
            to_mate(x_peer(dx) * nc + c).wait_send()

    for h in range(PARTS):
        whole = pbuf.at[h, pl.ds(0, n_gx - 1)]
        pltpu.make_async_copy(whole, whole, psend.at[h]).wait()


def solution(mesh):
    n_gx, n_gy = mesh.shape["gx"], mesh.shape["gy"]

    def shards(first_factor, second_factor, result_in, pivot_scale):
        rows, ka = first_factor.shape
        kb, cols = second_factor.shape
        inner = ka * n_gx
        part, nc, line, xn = rows // PARTS, kb // ka, n_gx // 2, n_gy // 2
        slot = -(-(part // LANES) // 8) * 8
        held = 2 * (rows * inner + inner * cols) + 4 * rows * cols
        dma = pltpu.SemaphoreType.DMA
        hbm = pl.BlockSpec(memory_space=pltpu.HBM)
        return pl.pallas_call(
            functools.partial(kernel, n_gx, n_gy),
            out_shape=jax.ShapeDtypeStruct((rows, cols), jnp.float32),
            in_specs=[hbm] * 4,
            out_specs=pl.BlockSpec(memory_space=pltpu.VMEM),
            scratch_shapes=[
                pltpu.VMEM((n_gx, PARTS, part, ka), jnp.bfloat16),
                pltpu.VMEM((n_gx, ka, cols), jnp.bfloat16),
                pltpu.VMEM((PARTS, n_gx, slot, LANES), jnp.float32),
                pltpu.VMEM((1, inner), jnp.float32),
                dma((PARTS,)), dma((nc,)), dma, dma,
                dma((n_gx, PARTS)), dma((n_gx,)),
                dma((line, PARTS)), dma((PARTS,)), dma((line, PARTS)), dma((PARTS,)),
                dma((n_gx,)), dma((max(xn - 1, 1) * nc,)),
                dma((PARTS,)), dma((PARTS,)),
            ],
            compiler_params=pltpu.CompilerParams(
                collective_id=0, has_side_effects=True, vmem_limit_bytes=held + 8 * 2**20),
        )(*[pltpu.with_memory_space_constraint(v, pltpu.HBM) for v in (first_factor, second_factor, result_in, pivot_scale.reshape(1, inner))])

    return jax.shard_map(
        shards,
        mesh=mesh,
        in_specs=(P("gy", "gx"), P("gy", "gx"), P("gy", "gx"), P()),
        out_specs=P("gy", "gx"),
        check_vma=False,
    )
```
